128 devices in a mesh: node: 32 (over z, y, core), local: 4 (over x).
Axes of the slice: x: 4, y: 4, z: 4, core: 2. Of those that a mesh axis runs over, the one named last changes fastest.
Arguments:
- tokens: bfloat16 [16384, 4096], P(('node', 'local')), may hold values from -6 to 6
- expert_ids: int32 [16384, 8], P(('node', 'local')), may hold values from 0 to 127, all different within a row; in each aligned block of 128 rows (0 to 127, 128 to 255, ...) at most 10 rows name the same one
- gate_scores: float32 [16384, 8], P(('node', 'local')), may hold values from 0.03 to 0.4
- w_gate: bfloat16 [128, 4096, 768], P(('node', 'local')), may hold values from -0.09375 to 0.09375
- w_up: bfloat16 [128, 4096, 768], P(('node', 'local')), may hold values from -0.09375 to 0.09375
- w_down: bfloat16 [128, 768, 4096], P(('node', 'local')), may hold values from -0.21875 to 0.21875
Outputs:
- mixed: bfloat16 [16384, 4096], P(('node', 'local'))
The draws below stay inside these ranges and needn't reach their ends.
Inputs may be any that keep to these rules, and one draw needn't show every extreme that they name: `expert_ids`: each row names 8 different experts. Among the 128 rows of one device no expert is named more than 10 times, and that many is reached on some device.
All inputs are finite; a program needn't handle non-finite values.
Results may differ from the reference program's by a relative error of at most 0.0058.
Values may be sent and summed in bfloat16 or wider, within the bound.
A program may use at most 128 MiB of HBM per device.

```python
import math
import jax
import jax.numpy as jnp
import numpy as np
from jax import lax

D = 4096
FF = 768
TOP = 8
TOK_DEV = 128
EXPERTS = 128
CAP = 10
TOKENS = 16384


def level_of(stream_key, extent, shards, least, largest):
    def one(position, parts):
        steps = jax.random.uniform(jax.random.fold_in(jax.random.fold_in(stream_key, 6), position), (parts,), jnp.float32, least / len(shards), largest / len(shards))
        return jnp.repeat(jnp.exp(steps), extent[position] // parts).reshape((-1,) + (1,) * (len(extent) - position - 1))

    factor_of = one(*shards[0])
    for cut in shards[1:]:
        factor_of = factor_of * one(*cut)
    return factor_of


def routed_block(rng, own, number, rows, number_of, top, limit, lean):
    ranking = jax.random.permutation(rng, number_of)
    packed, ordinary = shares(number_of, rows * top, limit, lean, True), shares(number_of, rows * top, limit, lean, False)
    places = jnp.arange(number_of)

    def named(sizes, turn):
        used = int((sizes > 0).sum())
        fixed = max(1, used // 4)
        moved = fixed + (places - fixed + turn * (used - fixed)) % max(1, number_of - fixed)
        return jnp.zeros((number_of,), jnp.int32).at[ranking[jnp.where(places < fixed, places, moved)]].set(jnp.asarray(sizes, jnp.int32))

    sizes = jnp.where(number % 4 == 0, named(packed, number // 4), named(ordinary, number - number // 4 - 1))
    mixed = jax.random.permutation(jax.random.fold_in(own, 3), number_of)
    donor, receiver = mixed[0:number_of // 2 * 2:2], mixed[1:number_of // 2 * 2:2]
    slack = jnp.minimum(sizes[donor] - 1, limit - sizes[receiver]) // 2
    slack = jnp.where((donor == ranking[0]) | (receiver == ranking[0]) | (sizes[receiver] == 0), 0, jnp.maximum(slack, 0))
    moved = jax.random.randint(jax.random.fold_in(own, 4), (number_of // 2,), 0, 1 << 20) % (slack + 1)
    sizes = sizes.at[donor].add(-moved).at[receiver].add(moved)
    items = jnp.searchsorted(jnp.cumsum(sizes), jnp.arange(rows * top), side="right").astype(jnp.int32)
    grid = items.reshape(top, rows).T
    grid = grid[jax.random.permutation(jax.random.fold_in(own, 1), rows)]
    turn = jax.random.randint(jax.random.fold_in(own, 2), (rows, 1), 0, top)
    return jnp.take_along_axis(grid, (jnp.arange(top)[None, :] + turn) % top, axis=1)


def shares(amount, total, limit, skew, full):
    loads = [(1 << 20) // math.isqrt(grade ** skew) + 1 for grade in range(1, amount + 1)]
    largest = limit if full else min(limit, max(-(-total // amount), total * loads[0] // sum(loads)))
    least = 1 if total - largest >= amount - 1 else 0
    holding, surplus = [largest] + [least] * (amount - 1), total - largest - least * (amount - 1)
    while surplus > 0:
        candidates = [i for i in range(1, amount) if holding[i] < largest] or [i for i in range(1, amount) if holding[i] < limit]
        whole, budget = sum([loads[i] for i in candidates]), surplus
        for i in candidates:
            extra = min(limit - holding[i], max(1, budget * loads[i] // whole), surplus)
            holding[i] = holding[i] + extra
            surplus = surplus - extra
    return np.array(holding)


def normal_values(rng, extent, scale, reach, cuts=(), held_as=jnp.bfloat16):
    entries = jax.random.normal(rng, extent, jnp.float32) * scale
    if len(cuts) > 0:
        entries = level_of(rng, extent, cuts, -0.22, 0.18) * entries
    return jnp.clip(entries, min=-reach, max=reach).astype(held_as)


def setup_inputs(seed: int = 0) -> dict:
    key_list = jax.random.split(jax.random.key(seed), 7)
    tokens = normal_values(key_list[0], (TOKENS, D), 1.0, 6.0, ((0, 128),))
    expert_ids_keys = jax.random.split(jax.random.fold_in(key_list[1], 1), TOKENS // TOK_DEV)
    expert_ids_turns = jax.random.permutation(jax.random.fold_in(key_list[1], 3), TOKENS // TOK_DEV)
    expert_ids = jax.vmap(lambda own, number: routed_block(jax.random.fold_in(key_list[1], 2), own, number, TOK_DEV, EXPERTS, TOP, CAP, 1))(expert_ids_keys, expert_ids_turns).reshape((TOKENS, TOP))
    gate_scores = jnp.clip(jnp.exp(math.log(0.4) - 2.5902672 * jax.random.uniform(key_list[2], (TOKENS, TOP), jnp.float32) ** level_of(key_list[2], (TOKENS, TOP), ((0, 128),), -0.2, 0.2)), 0.03, 0.4)
    w_gate = normal_values(key_list[3], (EXPERTS, D, FF), D ** -0.5, 0.09375, ((0, 128),))
    w_up = normal_values(key_list[4], (EXPERTS, D, FF), D ** -0.5, 0.09375, ((0, 128),))
    w_down = normal_values(key_list[5], (EXPERTS, FF, D), FF ** -0.5, 0.21875, ((0, 128),))
    return dict(tokens=tokens, expert_ids=expert_ids, gate_scores=gate_scores, w_gate=w_gate, w_up=w_up, w_down=w_down)


def reference(tokens, expert_ids, gate_scores, w_gate, w_up, w_down):
    flat_ids = expert_ids.reshape(-1)
    flat_gates = gate_scores.reshape(-1)
    slot_limit = EXPERTS * CAP

    def add_expert(totals, expert):
        chosen = flat_ids == expert
        positions = jnp.nonzero(chosen, size=slot_limit, fill_value=0)[0].astype(jnp.int32)
        live_rows = jnp.arange(slot_limit, dtype=jnp.int32) < jnp.sum(chosen.astype(jnp.int32))
        token_rows = positions // TOP
        inputs = tokens[token_rows]
        gate_part = jnp.dot(inputs, w_gate[expert], preferred_element_type=jnp.float32)
        up_part = jnp.dot(inputs, w_up[expert], preferred_element_type=jnp.float32)
        hidden = (jax.nn.silu(gate_part) * up_part).astype(jnp.bfloat16)
        output = jnp.dot(hidden, w_down[expert], preferred_element_type=jnp.float32).astype(jnp.bfloat16).astype(jnp.float32)
        weights = jnp.where(live_rows, flat_gates[positions], jnp.zeros((), jnp.float32))
        totals = totals.at[token_rows].add(weights[:, None] * output)
        return totals, None

    start = jnp.zeros((TOKENS, D), jnp.float32)
    totals, unused = lax.scan(add_expert, start, jnp.arange(EXPERTS, dtype=jnp.int32))
    return totals.astype(jnp.bfloat16)
```

```python
import jax
import jax.numpy as jnp
from jax import lax
from jax.sharding import PartitionSpec as P

MAIN = 8
FOLD = 4


def per_device(tokens, expert_ids, gate_scores, w_gate, w_up, w_down):
    axes = ("node", "local")
    experts = lax.axis_size("node") * lax.axis_size("local")
    token_count, features = tokens.shape
    quarter = features // FOLD
    f32, bf16 = jnp.float32, jnp.bfloat16

    expert_range = jnp.arange(experts, dtype=jnp.int32)
    match = expert_ids[:, :, None] == expert_range[None, None, :]
    chosen = jnp.any(match, axis=1)
    weight = jnp.sum(jnp.where(match, gate_scores[:, :, None], 0.0), axis=1)
    row = lax.broadcasted_iota(jnp.int32, (token_count, token_count), 0)
    col = lax.broadcasted_iota(jnp.int32, (token_count, token_count), 1)
    rank = jnp.dot((col < row).astype(bf16), chosen.astype(bf16), preferred_element_type=f32)
    rank = jnp.where(chosen, rank.astype(jnp.int32), -1)
    rank_t = rank.T

    sub = jnp.arange(MAIN, dtype=jnp.int32)
    pick_main = (rank_t[:, None, :] == sub[None, :, None]).astype(bf16)
    pick_main = pick_main.reshape(experts * MAIN, token_count)
    fold_hit = rank_t[:, None, :] == (MAIN + sub // FOLD)[None, :, None]
    fold_of = sub % FOLD
    main = jnp.dot(pick_main, tokens, preferred_element_type=f32).astype(bf16)
    extra = jnp.zeros((experts * MAIN, quarter), f32)
    for part in range(FOLD):
        pick = (fold_hit & (fold_of == part)[None, :, None]).astype(bf16)
        extra = extra + jnp.dot(
            pick.reshape(experts * MAIN, token_count),
            tokens[:, part * quarter : (part + 1) * quarter],
            preferred_element_type=f32,
        )
    extra = extra.astype(bf16)

    def exchange(block, width):
        block = block.reshape(experts, MAIN, width)
        return lax.all_to_all(block, axes, split_axis=0, concat_axis=0, tiled=True).reshape(
            experts * MAIN, width
        )

    main = exchange(main, features)
    extra = exchange(extra, quarter)

    over = MAIN // FOLD * experts
    over_row = lax.broadcasted_iota(jnp.int32, (over, experts * MAIN), 0)
    sub_row = lax.broadcasted_iota(jnp.int32, (over, experts * MAIN), 1)
    folds = [(sub_row == FOLD * over_row + part).astype(bf16) for part in range(FOLD)]
    extra_rows = jnp.concatenate(
        [jnp.dot(f, extra, preferred_element_type=f32).astype(bf16) for f in folds], axis=1
    )

    def expert(rows):
        gate_part = jnp.dot(rows, w_gate[0], preferred_element_type=f32)
        up_part = jnp.dot(rows, w_up[0], preferred_element_type=f32)
        hidden = (jax.nn.silu(gate_part) * up_part).astype(bf16)
        return jnp.dot(hidden, w_down[0], preferred_element_type=f32).astype(bf16)

    main = expert(main)
    extra_rows = expert(extra_rows)
    extra = jnp.zeros((experts * MAIN, quarter), f32)
    for part in range(FOLD):
        extra = extra + jnp.dot(
            folds[part].T,
            extra_rows[:, part * quarter : (part + 1) * quarter],
            preferred_element_type=f32,
        )
    extra = extra.astype(bf16)

    main = exchange(main, features)
    extra = exchange(extra, quarter)

    high = lax.reduce_precision(weight, 8, 7)
    parts = jnp.concatenate([high, weight - high], axis=0).astype(bf16)
    rank2 = jnp.concatenate([rank, rank], axis=0)
    put_main = jnp.where(rank2[:, :, None] == sub[None, None, :], parts[:, :, None], 0)
    put_main = put_main.reshape(2 * token_count, experts * MAIN).astype(bf16)
    put_hit = rank2[:, :, None] == (MAIN + sub // FOLD)[None, None, :]
    total = jnp.dot(put_main, main, preferred_element_type=f32)
    cols = []
    for part in range(FOLD):
        put = jnp.where(put_hit & (fold_of == part)[None, None, :], parts[:, :, None], 0)
        put = put.reshape(2 * token_count, experts * MAIN).astype(bf16)
        cols.append(jnp.dot(put, extra, preferred_element_type=f32))
    total = total + jnp.concatenate(cols, axis=1)
    return (total[:token_count] + total[token_count:]).astype(bf16)


def solution(mesh):
    in_specs = (
        P(("node", "local"), None),
        P(("node", "local"), None),
        P(("node", "local"), None),
        P(("node", "local"), None, None),
        P(("node", "local"), None, None),
        P(("node", "local"), None, None),
    )
    out_specs = P(("node", "local"), None)
    return jax.shard_map(
        per_device, mesh=mesh, in_specs=in_specs, out_specs=out_specs, check_vma=False
    )
```

```python
import jax
import jax.numpy as jnp
from jax import lax
from jax.sharding import PartitionSpec as P

MAIN = 8
FOLD = 4


def per_device(tokens, expert_ids, gate_scores, w_gate, w_up, w_down):
    axes = ("node", "local")
    experts = lax.axis_size("node") * lax.axis_size("local")
    token_count, features = tokens.shape
    quarter = features // FOLD
    slots = experts * MAIN
    f32, bf16 = jnp.float32, jnp.bfloat16

    expert_range = jnp.arange(experts, dtype=jnp.int32)
    match = expert_ids[:, :, None] == expert_range[None, None, :]
    chosen = jnp.any(match, axis=1)
    row = lax.broadcasted_iota(jnp.int32, (token_count, token_count), 0)
    col = lax.broadcasted_iota(jnp.int32, (token_count, token_count), 1)
    rank = jnp.dot((col < row).astype(bf16), chosen.astype(bf16), preferred_element_type=f32)
    rank = jnp.where(chosen, rank.astype(jnp.int32), -1)
    rank_t = rank.T

    sub = jnp.arange(MAIN, dtype=jnp.int32)
    fold_of = sub % FOLD
    part_range = jnp.arange(FOLD, dtype=jnp.int32)

    def exchange(block, width):
        block = block.reshape(experts, MAIN, width)
        return lax.all_to_all(block, axes, split_axis=0, concat_axis=0, tiled=True).reshape(
            slots, width
        )

    pick_main = (rank_t[:, None, :] == sub[None, :, None]).astype(bf16)
    main = jnp.dot(
        pick_main.reshape(slots, token_count), tokens, preferred_element_type=f32
    ).astype(bf16)
    main = exchange(main, features)

    fold_hit = rank_t[:, None, :] == (MAIN + sub // FOLD)[None, :, None]
    extra = jnp.zeros((slots, quarter), f32)
    for part in range(FOLD):
        pick = (fold_hit & (fold_of == part)[None, :, None]).astype(bf16)
        extra = extra + jnp.dot(
            pick.reshape(slots, token_count),
            tokens[:, part * quarter : (part + 1) * quarter],
            preferred_element_type=f32,
        )
    extra = extra.astype(bf16)
    extra, main = lax.optimization_barrier((extra, main))
    extra = exchange(extra, quarter)

    def expert(rows):
        gate_part = jnp.dot(rows, w_gate[0], preferred_element_type=f32)
        up_part = jnp.dot(rows, w_up[0], preferred_element_type=f32)
        hidden = (jax.nn.silu(gate_part) * up_part).astype(bf16)
        return jnp.dot(hidden, w_down[0], preferred_element_type=f32).astype(bf16)

    main = expert(main)
    main, extra = lax.optimization_barrier((main, extra))
    main_back = exchange(main, features)

    over = MAIN // FOLD * experts
    over_row = lax.broadcasted_iota(jnp.int32, (over, slots), 0)
    sub_row = lax.broadcasted_iota(jnp.int32, (over, slots), 1)
    folds = [(sub_row == FOLD * over_row + part).astype(bf16) for part in range(FOLD)]
    extra_rows = jnp.concatenate(
        [jnp.dot(f, extra, preferred_element_type=f32).astype(bf16) for f in folds], axis=1
    )
    extra_rows = expert(extra_rows)
    extra = jnp.zeros((slots, quarter), f32)
    for part in range(FOLD):
        extra = extra + jnp.dot(
            folds[part].T,
            extra_rows[:, part * quarter : (part + 1) * quarter],
            preferred_element_type=f32,
        )
    extra = extra.astype(bf16)

    weight = jnp.sum(jnp.where(match, gate_scores[:, :, None], 0.0), axis=1)
    put_main = jnp.where(rank[:, :, None] == sub[None, None, :], weight[:, :, None], 0.0)
    put_main = put_main.astype(bf16).reshape(token_count, slots)
    put_hit = rank[:, :, None] == (MAIN + sub // FOLD)[None, None, :]
    put_extra = jnp.where(
        put_hit[None] & (fold_of[None, :] == part_range[:, None])[:, None, None, :],
        weight[None, :, :, None],
        0.0,
    )
    put_extra = put_extra.astype(bf16).reshape(FOLD * token_count, slots)

    extra, main_back, put_extra, put_main = lax.optimization_barrier(
        (extra, main_back, put_extra, put_main)
    )
    extra_back = exchange(extra, quarter)

    total = jnp.dot(put_main, main_back, preferred_element_type=f32)
    total, extra_back = lax.optimization_barrier((total, extra_back))
    quarters = jnp.dot(put_extra, extra_back, preferred_element_type=f32)
    quarters = quarters.reshape(FOLD, token_count, quarter)
    total = total + jnp.concatenate([quarters[part] for part in range(FOLD)], axis=1)
    return total.astype(bf16)


def solution(mesh):
    in_specs = (
        P(("node", "local"), None),
        P(("node", "local"), None),
        P(("node", "local"), None),
        P(("node", "local"), None, None),
        P(("node", "local"), None, None),
        P(("node", "local"), None, None),
    )
    out_specs = P(("node", "local"), None)
    return jax.shard_map(
        per_device, mesh=mesh, in_specs=in_specs, out_specs=out_specs, check_vma=False
    )
```
